256 devices in a mesh: leaf: 256 (over x, y, z, core).
Axes of the slice: x: 4, y: 4, z: 8, core: 2. Of those that a mesh axis runs over, the one named last changes fastest.
Arguments:
- coarse_basis: float32 [9, 131072, 256], P(None, 'leaf'), as said below
- rhs_vectors_coarse: float32 [131072, 768], P('leaf'), may hold values from -6 to 6
- vertex_tier_depth: int32 [131072], P('leaf'), may hold values from 0 to 8
Outputs:
- solution: float32 [131072, 768], P('leaf')
The draws below stay inside these ranges and needn't reach their ends.
Inputs may be any that keep to these rules, and one draw needn't show every extreme that they name: vertex_tier_depth[v] is the coarsest separator level whose block has vertex v in its support; level 0 is the vertex's own leaf block. `coarse_basis`: float32 entries, finite.
All inputs are finite; a program needn't handle non-finite values.
Results may differ from the reference program's by a relative error of at most 0.0001.
Values sent between devices are 32-bit elements; how exact they have to be, the bound alone decides.
A program may use at most 128 MiB of HBM per device.

```python
import jax
import jax.numpy as jnp
from jax import lax

S = 256
V_DEV = 512
NRHS = 768
LEVELS = 8
VERTS = 131072
N_LEAF = 256


def draw_coarse_basis(key, part):
    level_number = jnp.arange(LEVELS + 1).astype(jnp.float32)
    tier_scale_factor = (S * V_DEV * jnp.exp2(level_number)) ** (-0.25)
    entries = jax.random.normal(key, (LEVELS + 1, VERTS, S), jnp.float32)
    return (entries * tier_scale_factor[:, None, None]).astype(jnp.float32)


def set_ends(array, stream_key, least, largest):
    extent = array.shape
    place = [jax.random.randint(jax.random.fold_in(stream_key, axis), (), 0, extent[axis]) for axis in range(len(extent))]
    array = array.at[tuple(place)].set(least)
    longest = extent.index(max(extent))
    place[longest] = (place[longest] + 1) % extent[longest]
    return array.at[tuple(place)].set(largest)


def level_of(stream_key, dims, cuts, low, top_value):
    loudness = 1.0
    for dim, parts in cuts:
        heights = jax.random.uniform(jax.random.fold_in(jax.random.fold_in(stream_key, 6), dim), (parts,), jnp.float32, low / len(cuts), top_value / len(cuts))
        loudness = loudness * jnp.repeat(jnp.exp(heights), dims[dim] // parts).reshape((-1,) + (1,) * (len(dims) - 1 - dim))
    return loudness


def centred(rng, extent, scale, most, pieces=(), kind=jnp.bfloat16):
    gain = level_of(rng, extent, pieces, -0.22, 0.18) if pieces else 1.0
    drawn = jax.random.normal(rng, extent, jnp.float32) * scale * gain
    return jnp.minimum(jnp.maximum(drawn, -most), most).astype(kind)


def setup_inputs(seed: int = 0) -> dict:
    key_list = jax.random.split(jax.random.key(seed), 4)
    coarse_basis = draw_coarse_basis(jax.random.fold_in(key_list[3], 71), 0)
    rhs_vectors_coarse = centred(key_list[1], (VERTS, NRHS), 1.0, 6.0, ((0, 256),), jnp.float32)
    vertex_tier_depth = set_ends(jax.random.randint(key_list[2], (VERTS,), 0, LEVELS + 1), jax.random.fold_in(key_list[2], 1), 0, LEVELS).astype(jnp.int32)
    return {"coarse_basis": coarse_basis, "rhs_vectors_coarse": rhs_vectors_coarse, "vertex_tier_depth": vertex_tier_depth}


def reference(coarse_basis, rhs_vectors_coarse, vertex_tier_depth):
    vertex_count = coarse_basis.shape[1]
    solution = jnp.zeros((vertex_count, NRHS), jnp.float32)
    for level_number in range(LEVELS + 1):
        level_mask = (vertex_tier_depth >= level_number).astype(jnp.float32)
        level_basis = coarse_basis[level_number] * level_mask[:, None]
        group_count = N_LEAF // (2 ** level_number)
        grouped_basis = level_basis.reshape(group_count, -1, S)
        grouped_sides = rhs_vectors_coarse.reshape(group_count, -1, NRHS)
        coefficients = jnp.einsum("gvs,gvr->gsr", grouped_basis, grouped_sides, precision=lax.Precision.HIGHEST)
        image = jnp.einsum("gvs,gsr->gvr", grouped_basis, coefficients, precision=lax.Precision.HIGHEST)
        solution = solution + image.reshape(vertex_count, NRHS)
    return solution
```

```python
import functools

import jax
import jax.numpy as jnp
from jax import lax
from jax.experimental import pallas as pl
from jax.experimental.pallas import tpu as pltpu
from jax.sharding import PartitionSpec as P

MESH = pl.DeviceIdType.MESH
F32, BF16 = jnp.float32, jnp.bfloat16

S, V, R = 256, 512, 768
HALF = R // 2
NX, NY, NZ = 4, 4, 8
LEVELS = 9
RECV_ROWS, N_SEND, N_RECV = 6400, 128, 128

ORDER = [8, 4, 8, 7, 4, 5, 7, 8, 6, 4, 5, 3, 6, 7, 8, 4, 2, 5, 3, 6, 7, 8, 4, 2, 5, 1, 3, 6, 7, 8, 4, 0, 5, 1,
         3, 6, 7, 8, 4, 0, 2, 5, 3, 6, 7, 8, 4, 2, 5, 3, 6, 7, 8, 4, 5, 7, 8, 4, 5, 4, 5, 5, 5]


def split(x):
    hi = x.astype(BF16)
    return hi, (x - hi.astype(F32)).astype(BF16)


def aligned(offset, by=8):
    return offset if isinstance(offset, int) else pl.multiple_of(offset, by)


class Exchange:
    def __init__(self, part, coef, recv, send_sem, recv_sem, me):
        self.part, self.coef, self.recv = part, coef, recv
        self.send_sem, self.recv_sem, self.me = send_sem, recv_sem, me
        self.rows = self.sends = self.recvs = 0
        self.started = []

    def slots(self, n, rows):
        first, sem = self.rows, self.recvs
        self.rows += n * rows
        self.recvs += n
        assert self.rows <= RECV_ROWS and self.recvs <= N_RECV
        return first, sem

    def sems(self, n):
        sem = self.recvs
        self.recvs += n
        assert self.recvs <= N_RECV
        return sem

    def at(self, ref, level, offset, rows):
        offset = aligned(offset)
        return ref.at[pl.ds(offset, rows)] if level is None else ref.at[level, pl.ds(offset, rows)]

    def send(self, src, dst, sem, device, when=None):
        copy = pltpu.make_async_remote_copy(
            src_ref=src, dst_ref=dst, send_sem=self.send_sem.at[self.sends], recv_sem=self.recv_sem.at[sem],
            device_id=(device,), device_id_type=MESH)
        self.sends += 1
        assert self.sends <= N_SEND
        self.started.append((copy, when))
        if when is None:
            copy.start()
        else:
            pl.when(when)(copy.start)

    def wait(self, dst, sem, device):
        pltpu.make_async_remote_copy(
            src_ref=dst, dst_ref=dst, send_sem=self.send_sem.at[0], recv_sem=self.recv_sem.at[sem],
            device_id=(device,), device_id_type=MESH).wait_recv()

    def drain(self):
        for copy, when in self.started:
            if when is None:
                copy.wait_send()
            else:
                pl.when(when)(copy.wait_send)


def kernel(basis, rhs, depth, out, bas_v, rhs_v, x_hi, x_lo, b_hi, b_lo, tier, part, coef, recv, acc,
           load_sem, store_sem, send_sem, recv_sem):
    me = lax.axis_index("leaf")
    core = lax.rem(me, 2)
    z = lax.rem(me // 2, NZ)
    y = lax.rem(me // (2 * NZ), NY)
    x = me // (2 * NZ * NY)

    def at_core(c):
        return me - core + c

    def at_z(k):
        return me + 2 * (k - z)

    def at_y(k):
        return me + 2 * NZ * (k - y)

    def at_x(k):
        return me + 2 * NZ * NY * (k - x)

    barrier = pltpu.get_barrier_semaphore()
    partners = [at_core(1 - core)]
    partners += [at_z(lax.rem(z + d, NZ)) for d in range(1, NZ)]
    partners += [at_y(lax.rem(y + d, NY)) for d in range(1, NY)]
    partners += [at_x(lax.rem(x + d, NX)) for d in range(1, NX)]
    for partner in partners:
        pl.semaphore_signal(barrier, inc=1, device_id=(partner,), device_id_type=MESH)

    first_seen = list(dict.fromkeys(ORDER))
    load_rhs = pltpu.make_async_copy(rhs, rhs_v, load_sem.at[LEVELS])
    load_rhs.start()
    loads = {}
    for level in first_seen:
        loads[level] = pltpu.make_async_copy(basis.at[level], bas_v.at[level], load_sem.at[level])
        loads[level].start()

    for k in range(V // 128):
        row = depth[0:1, 128 * k:128 * (k + 1)].astype(F32)
        tier[128 * k:128 * (k + 1), :] = jnp.broadcast_to(row, (128, 128)).T

    load_rhs.wait()
    for k in range(R // 128):
        hi, lo = split(rhs_v[:, 128 * k:128 * (k + 1)].T)
        b_hi[128 * k:128 * (k + 1), :] = hi
        b_lo[128 * k:128 * (k + 1), :] = lo

    ex = Exchange(part, coef, recv, send_sem, recv_sem, me)
    mine = core * HALF

    def project(level):
        loads[level].wait()
        for k in range(S // 128):
            cols = slice(128 * k, 128 * (k + 1))
            kept = jnp.where(tier[...] >= float(level), bas_v[level, :, cols], 0.0)
            hi, lo = split(kept)
            x_hi[level, :, cols] = hi
            x_lo[level, :, cols] = lo
        hi, lo = x_hi[level], x_lo[level]
        part[level] = (jnp.dot(b_hi[...], hi, preferred_element_type=F32)
                       + jnp.dot(b_hi[...], lo, preferred_element_type=F32)
                       + jnp.dot(b_lo[...], hi, preferred_element_type=F32))

    def nt(a, b):
        return lax.dot_general(a, b, (((1,), (1,)), ((), ())), preferred_element_type=F32)

    state = {"applied": 0}
    stores = []

    def apply(level, coefficients):
        hi, lo = split(coefficients)
        first, last = state["applied"] == 0, state["applied"] == LEVELS - 1
        state["applied"] += 1
        if not last:
            image = nt(x_hi[level], hi) + nt(x_hi[level], lo) + nt(x_lo[level], hi)
            acc[...] = image if first else acc[...] + image
            return
        for k in range(4):
            rows = slice(k * V // 4, (k + 1) * V // 4)
            image = nt(x_hi[level, rows], hi) + nt(x_hi[level, rows], lo) + nt(x_lo[level, rows], hi)
            acc[rows, :] = acc[rows, :] + image
            stores.append(pltpu.make_async_copy(acc.at[rows], out.at[rows], store_sem.at[k]))
            stores[-1].start()

    def add_into(level, offset, rows, slots):
        where = pl.ds(aligned(offset), rows)
        total = part[level, where, :]
        for slot in slots:
            total = total + recv[pl.ds(slot, rows), :]
        part[level, where, :] = total

    def cores_in(level):
        first, sem = ex.slots(1, HALF)
        other = at_core(1 - core)
        ex.send(ex.at(part, level, HALF - mine, HALF), ex.at(recv, None, first, HALF), sem, other)
        yield
        ex.wait(ex.at(recv, None, first, HALF), sem, other)
        add_into(level, mine, HALF, [first])

    def cores_out(level):
        sem = ex.sems(1)
        other = at_core(1 - core)
        ex.send(ex.at(coef, level, mine, HALF), ex.at(coef, level, mine, HALF), sem, other)
        yield
        ex.wait(ex.at(coef, level, HALF - mine, HALF), sem, other)

    def pair_in(level, base, rows, bit, other):
        first, sem = ex.slots(1, rows)
        ex.send(ex.at(part, level, base + (1 - bit) * rows, rows), ex.at(recv, None, first, rows), sem, other)
        yield
        ex.wait(ex.at(recv, None, first, rows), sem, other)
        add_into(level, base + bit * rows, rows, [first])

    def pair_out(level, base, rows, bit, other):
        sem = ex.sems(1)
        block = ex.at(coef, level, base + bit * rows, rows)
        ex.send(block, block, sem, other)
        yield
        ex.wait(ex.at(coef, level, base + (1 - bit) * rows, rows), sem, other)

    def four_in(level, base, rows, pos, device):
        first, sem = ex.slots(3, rows)
        for d in range(1, 4):
            to = lax.rem(pos + d, 4)
            ex.send(ex.at(part, level, base + to * rows, rows), ex.at(recv, None, first + (d - 1) * rows, rows),
                    sem + d - 1, device(to))
        yield
        for d in range(1, 4):
            ex.wait(ex.at(recv, None, first + (d - 1) * rows, rows), sem + d - 1, device(lax.rem(pos + 4 - d, 4)))
        add_into(level, base + pos * rows, rows, [first + d * rows for d in range(3)])

    def four_out(level, base, rows, pos, device):
        sem = ex.sems(3)
        block = ex.at(coef, level, base + pos * rows, rows)
        for d in range(1, 4):
            ex.send(block, block, sem + d - 1, device(lax.rem(pos + d, 4)))
        yield
        for d in range(1, 4):
            source = lax.rem(pos + 4 - d, 4)
            ex.wait(ex.at(coef, level, base + source * rows, rows), sem + d - 1, device(source))

    def roots_sum(level, base, rows, count):
        if count == 3:
            places = [2 * r for r in range(3)]
            is_root, my_root = jnp.logical_and(lax.rem(z, 2) == 0, z < 6), z // 2
        else:
            places = [r + r // 3 for r in range(6)]
            is_root, my_root = lax.rem(z, 4) != 3, z - z // 4
        first, sem = ex.slots(NZ - 1, rows)
        for r, place in enumerate(places):
            slot = lax.rem(z - place + NZ, NZ) - 1
            slot = jnp.maximum(slot, 0)
            ex.send(ex.at(part, level, base + r * rows, rows), ex.at(recv, None, first + slot * rows, rows),
                    sem + slot, at_z(place), when=z != place)
        yield
        back = ex.sems(count)
        where = base + my_root * rows

        @pl.when(is_root)
        def _():
            for d in range(1, NZ):
                ex.wait(ex.at(recv, None, first + (d - 1) * rows, rows), sem + d - 1, at_z(lax.rem(z + d, NZ)))
            total = part[level, pl.ds(aligned(where), rows), :]
            for d in range(NZ - 1):
                total = total + recv[pl.ds(first + d * rows, rows), :]
            coef[level, pl.ds(aligned(where), rows), :] = total

        block = ex.at(coef, level, jnp.where(is_root, where, base), rows)
        sem_at = back + jnp.where(is_root, my_root, 0)
        for d in range(1, NZ):
            ex.send(block, block, sem_at, at_z(lax.rem(z + d, NZ)), when=is_root)
        yield
        for r, place in enumerate(places):
            @pl.when(z != place)
            def _():
                ex.wait(ex.at(coef, level, base + r * rows, rows), back + r, at_z(place))

    def chain_sum(level, base, rows):
        cut = rows // 16 * 8
        up, down = at_z(lax.rem(z + 1, NZ)), at_z(lax.rem(z + NZ - 1, NZ))

        def block(d):
            return base + lax.rem(z + d + NZ, NZ) * rows

        for step in range(1, 5):
            far = 5 - step
            n_up, n_down, skip = (cut, rows - cut, cut) if step == 1 else (rows, rows, 0)
            first, sem = ex.slots(1, n_up)
            first_down, sem_down = ex.slots(1, n_down)
            ex.send(ex.at(part, level, block(far), n_up), ex.at(recv, None, first, n_up), sem, up)
            ex.send(ex.at(part, level, block(-far) + skip, n_down), ex.at(recv, None, first_down, n_down), sem_down, down)
            yield
            ex.wait(ex.at(recv, None, first, n_up), sem, down)
            ex.wait(ex.at(recv, None, first_down, n_down), sem_down, up)
            if step < 4:
                add_into(level, block(far - 1), n_up, [first])
                add_into(level, block(1 - far) + skip, n_down, [first_down])
        own = pl.ds(aligned(block(0)), rows)
        coef[level, own, :] = part[level, own, :] + recv[pl.ds(first, rows), :] + recv[pl.ds(first_down, rows), :]
        for step in range(1, 5):
            n_up, n_down, skip = (cut, rows - cut, cut) if step == 4 else (rows, rows, 0)
            sem = ex.sems(2)
            going_up = ex.at(coef, level, block(1 - step), n_up)
            going_down = ex.at(coef, level, block(step - 1) + skip, n_down)
            ex.send(going_up, going_up, sem, up)
            ex.send(going_down, going_down, sem + 1, down)
            yield
            ex.wait(ex.at(coef, level, block(-step), n_up), sem, down)
            ex.wait(ex.at(coef, level, block(step) + skip, n_down), sem + 1, up)

    def quad_sum(level, base):
        rows = HALF // 2
        place = lax.rem(z, 4)
        side = place // 2
        start = z - place
        middle = jnp.logical_or(place == 1, place == 2)
        edge = jnp.logical_not(middle)
        my_middle, my_edge, far_middle = at_z(start + 1 + side), at_z(start + 3 * side), at_z(start + 2 - side)
        near, far = base + side * rows, base + (1 - side) * rows
        first, sem = ex.slots(3, rows)
        back = ex.sems(2)
        slot = [ex.at(recv, None, first + k * rows, rows) for k in range(3)]
        ex.send(ex.at(part, level, far, rows), slot[0], sem, my_middle, when=edge)
        ex.send(ex.at(part, level, near, rows), slot[1], sem + 1, my_middle, when=edge)
        yield

        @pl.when(middle)
        def _():
            ex.wait(slot[0], sem, my_edge)
            add_into(level, far, rows, [first])

        ex.send(ex.at(part, level, far, rows), slot[2], sem + 2, far_middle, when=middle)
        yield

        @pl.when(middle)
        def _():
            ex.wait(slot[1], sem + 1, my_edge)
            ex.wait(slot[2], sem + 2, far_middle)
            where = pl.ds(aligned(near), rows)
            coef[level, where, :] = (part[level, where, :] + recv[pl.ds(first + rows, rows), :]
                                     + recv[pl.ds(first + 2 * rows, rows), :])

        block, other = ex.at(coef, level, near, rows), ex.at(coef, level, far, rows)
        ex.send(block, block, back, far_middle, when=middle)
        ex.send(block, block, back + 1, my_edge, when=middle)
        yield

        @pl.when(middle)
        def _():
            ex.wait(other, back, far_middle)

        ex.send(other, other, back, my_edge, when=middle)
        yield

        @pl.when(edge)
        def _():
            ex.wait(block, back + 1, my_middle)
            ex.wait(other, back, my_middle)

    def level_0():
        project(0)
        yield
        apply(0, part[0])

    def level_1():
        project(1)
        first, sem = ex.slots(1, R)
        other = at_core(1 - core)
        ex.send(part.at[1], ex.at(recv, None, first, R), sem, other)
        yield
        ex.wait(ex.at(recv, None, first, R), sem, other)
        apply(1, part[1] + recv[pl.ds(first, R), :])

    def level_2():
        project(2)
        yield from cores_in(2)
        first, sem = ex.slots(1, HALF)
        other = at_z(z + 1 - 2 * lax.rem(z, 2))
        ex.send(ex.at(part, 2, mine, HALF), ex.at(recv, None, first, HALF), sem, other)
        yield
        ex.wait(ex.at(recv, None, first, HALF), sem, other)
        own = pl.ds(aligned(mine), HALF)
        coef[2, own, :] = part[2, own, :] + recv[pl.ds(first, HALF), :]
        yield from cores_out(2)
        apply(2, coef[2])

    def level_3():
        project(3)
        yield from cores_in(3)
        yield from quad_sum(3, mine)
        yield from cores_out(3)
        apply(3, coef[3])

    def level_4():
        project(4)
        yield from cores_in(4)
        yield from chain_sum(4, mine, HALF // 8)
        yield from cores_out(4)
        apply(4, coef[4])

    def level_5():
        project(5)
        yield from cores_in(5)
        bit = lax.rem(y, 2)
        other = at_y(y + 1 - 2 * bit)
        yield from pair_in(5, mine, HALF // 2, bit, other)
        yield from chain_sum(5, mine + bit * (HALF // 2), HALF // 16)
        yield from pair_out(5, mine, HALF // 2, bit, other)
        yield from cores_out(5)
        apply(5, coef[5])

    def level_6():
        project(6)
        yield from cores_in(6)
        yield from four_in(6, mine, HALF // 4, y, at_y)
        yield from roots_sum(6, mine + y * (HALF // 4), HALF // 24, 6)
        yield from four_out(6, mine, HALF // 4, y, at_y)
        yield from cores_out(6)
        apply(6, coef[6])

    def level_7():
        project(7)
        yield from cores_in(7)
        bit = lax.rem(x, 2)
        other = at_x(x + 1 - 2 * bit)
        yield from pair_in(7, mine, HALF // 2, bit, other)
        base = mine + bit * (HALF // 2)
        yield from four_in(7, base, HALF // 8, y, at_y)
        yield from roots_sum(7, base + y * (HALF // 8), HALF // 48, 6)
        yield from four_out(7, base, HALF // 8, y, at_y)
        yield from pair_out(7, mine, HALF // 2, bit, other)
        yield from cores_out(7)
        apply(7, coef[7])

    def level_8():
        project(8)
        yield from cores_in(8)
        yield from four_in(8, mine, HALF // 4, x, at_x)
        base = mine + x * (HALF // 4)
        yield from four_in(8, base, HALF // 16, y, at_y)
        yield from roots_sum(8, base + y * (HALF // 16), HALF // 48, 3)
        yield from four_out(8, base, HALF // 16, y, at_y)
        yield from four_out(8, mine, HALF // 4, x, at_x)
        yield from cores_out(8)
        apply(8, coef[8])

    pl.semaphore_wait(barrier, len(partners))
    levels = [f() for f in (level_0, level_1, level_2, level_3, level_4, level_5, level_6, level_7, level_8)]
    for level in ORDER:
        next(levels[level], None)
    for level in (1, 2, 3, 6, 7, 8, 4, 5):
        for _ in levels[level]:
            pass
    assert state["applied"] == LEVELS
    ex.drain()
    for store in stores:
        store.wait()


def body(basis, rhs, depth):
    any_space = pl.BlockSpec(memory_space=pl.ANY)
    return pl.pallas_call(
        kernel,
        out_shape=jax.ShapeDtypeStruct((V, R), F32),
        in_specs=[any_space, any_space, pl.BlockSpec(memory_space=pltpu.VMEM)],
        out_specs=any_space,
        scratch_shapes=[
            pltpu.VMEM((LEVELS, V, S), F32),
            pltpu.VMEM((V, R), F32),
            pltpu.VMEM((LEVELS, V, S), BF16),
            pltpu.VMEM((LEVELS, V, S), BF16),
            pltpu.VMEM((R, V), BF16),
            pltpu.VMEM((R, V), BF16),
            pltpu.VMEM((V, 128), F32),
            pltpu.VMEM((LEVELS, R, S), F32),
            pltpu.VMEM((LEVELS, R, S), F32),
            pltpu.VMEM((RECV_ROWS, S), F32),
            pltpu.VMEM((V, R), F32),
            pltpu.SemaphoreType.DMA((LEVELS + 1,)),
            pltpu.SemaphoreType.DMA((4,)),
            pltpu.SemaphoreType.DMA((N_SEND,)),
            pltpu.SemaphoreType.DMA((N_RECV,)),
        ],
        compiler_params=pltpu.CompilerParams(
            collective_id=0, has_side_effects=True, vmem_limit_bytes=60 * 1024 * 1024),
        name="coarse_solve",
    )(basis, rhs, depth.reshape(1, V))


def solution(mesh):
    in_specs = (P(None, "leaf", None), P("leaf", None), P("leaf"))
    out_specs = P("leaf", None)
    return jax.shard_map(body, mesh=mesh, in_specs=in_specs, out_specs=out_specs, check_vma=False)
```

```python
import functools

import jax
import jax.numpy as jnp
from jax import lax
from jax.experimental import pallas as pl
from jax.experimental.pallas import tpu as pltpu
from jax.sharding import PartitionSpec as P

MESH = pl.DeviceIdType.MESH
F32, BF16 = jnp.float32, jnp.bfloat16

S, V, R = 256, 512, 768
HALF = R // 2
NX, NY, NZ = 4, 4, 8
LEVELS = 9
EARLY = 4
RECV_ROWS, N_SEND, N_RECV = 6400, 16, 112

ORDER = [5, 4, 7, 3, 6, 8, 5, 4, 1, 3, 30, 7, 2, 6, 4, 8, 5, 2, 6, 30, 23, 7, 5, 8, 4, 6, 20, 7, 5, 8, 6, 1, 7, 6, 5,
         8, 4, 8, 20, 6, 7, 6, 4, 0, 5, 8, 6, 31, 30, 7, 5, 6, 21, 7, 30, 8, 31, 6, 8, 4, 5, 7, 31, 6, 21, 0, 8, 5, 4,
         6, 31, 5, 30, 23, 8, 4, 22, 7, 6, 31, 7, 4, 6, 8, 3, 22, 5, 4, 8, 2, 5]


def split(x):
    hi = x.astype(BF16)
    return hi, (x - hi.astype(F32)).astype(BF16)


def aligned(offset, by=8):
    return offset if isinstance(offset, int) else pl.multiple_of(offset, by)


class Exchange:
    def __init__(self, recv, send_sem, recv_sem, other):
        self.recv, self.send_sem, self.recv_sem, self.other = recv, send_sem, recv_sem, other
        self.rows = self.sends = self.recvs = 0
        self.sent = {}

    def slots(self, rows):
        first = self.rows
        self.rows += rows
        assert self.rows <= RECV_ROWS
        return first

    def sem(self):
        self.recvs += 1
        assert self.recvs <= N_RECV
        return self.recv_sem.at[self.recvs - 1]

    def at(self, ref, level, offset, rows, cols=None):
        where = (pl.ds(aligned(offset), rows),)
        if cols is not None:
            where += (pl.ds(aligned(cols, 128), 128),)
        return ref.at[where] if level is None else ref.at[(level,) + where]

    def group(self, key):
        if key not in self.sent:
            assert self.sends < N_SEND
            self.sent[key] = [self.send_sem.at[self.sends], 0, None]
            self.sends += 1
        return self.sent[key]

    def send(self, src, dst, sem, device, key, when=None, drain=True):
        group = self.group(key)
        copy = pltpu.make_async_remote_copy(
            src_ref=src, dst_ref=dst, send_sem=group[0], recv_sem=sem, device_id=(device,), device_id_type=MESH)
        if drain:
            group[1] += src.shape[0] * src.shape[1] // 128
            group[2] = when
        if when is None:
            copy.start()
        else:
            pl.when(when)(copy.start)

    def whole(self, halves):
        if halves % 16:
            return self.recv.at[pl.ds(0, halves), pl.ds(0, 128)]
        return self.recv.at[pl.ds(0, halves // 2)]

    def descriptor(self, halves, send_sem, recv_sem):
        ref = self.whole(halves)
        return pltpu.make_async_remote_copy(
            src_ref=ref, dst_ref=ref, send_sem=send_sem, recv_sem=recv_sem, device_id=(self.other,),
            device_id_type=MESH)

    def wait(self, rows, sem, narrow=False):
        self.descriptor(rows if narrow else 2 * rows, self.send_sem.at[0], sem).wait_recv()

    def wait_sent(self, rows, sem):
        self.descriptor(2 * rows, sem, self.recv_sem.at[0]).wait_send()

    def drain(self):
        for sem, halves, when in self.sent.values():
            if halves:
                wait = self.descriptor(halves, sem, self.recv_sem.at[0]).wait_send
                wait() if when is None else pl.when(when)(wait)


def kernel(basis, rhs, depth, out, bas_v, rhs_v, x_hi, x_lo, b_hi, b_lo, tier, part, coef, recv, acc,
           load_sem, send_sem, recv_sem):
    me = lax.axis_index("leaf")
    core = lax.rem(me, 2)
    z = lax.rem(me // 2, NZ)
    y = lax.rem(me // (2 * NZ), NY)
    x = me // (2 * NZ * NY)

    def at_core(c):
        return me - core + c

    def at_z(k):
        return me + 2 * (k - z)

    def at_y(k):
        return me + 2 * NZ * (k - y)

    def at_x(k):
        return me + 2 * NZ * NY * (k - x)

    barrier = pltpu.get_barrier_semaphore()
    partners = [at_core(1 - core)]
    partners += [at_z(lax.rem(z + d, NZ)) for d in range(1, NZ)]
    partners += [at_y(lax.rem(y + d, NY)) for d in range(1, NY)]
    partners += [at_x(lax.rem(x + d, NX)) for d in range(1, NX)]
    for partner in partners:
        pl.semaphore_signal(barrier, inc=1, device_id=(partner,), device_id_type=MESH)

    first_seen = [level for level in dict.fromkeys(ORDER) if level < LEVELS]
    load_rhs = pltpu.make_async_copy(rhs, rhs_v, load_sem.at[LEVELS])
    load_rhs.start()
    loads = {}
    for level in first_seen:
        loads[level] = pltpu.make_async_copy(basis.at[level], bas_v.at[level], load_sem.at[level])
        loads[level].start()

    for k in range(V // 128):
        row = depth[0:1, 128 * k:128 * (k + 1)].astype(F32)
        tier[128 * k:128 * (k + 1), :] = jnp.broadcast_to(row, (128, 128)).T

    load_rhs.wait()
    for k in range(R // 128):
        hi, lo = split(rhs_v[:, 128 * k:128 * (k + 1)].T)
        b_hi[128 * k:128 * (k + 1), :] = hi
        b_lo[128 * k:128 * (k + 1), :] = lo

    ex = Exchange(recv, send_sem, recv_sem, at_core(1 - core))
    mine = core * HALF

    projected, prepared = set(), set()

    def prepare(level):
        if level in prepared:
            return
        prepared.add(level)
        loads[level].wait()
        for k in range(S // 128):
            cols = slice(128 * k, 128 * (k + 1))
            kept = jnp.where(tier[...] >= float(level), bas_v[level, :, cols], 0.0)
            hi, lo = split(kept)
            x_hi[level, :, cols] = hi
            x_lo[level, :, cols] = lo

    def project(level):
        if level in projected:
            return
        projected.add(level)
        prepare(level)
        if len(projected) < LEVELS:
            prepare(first_seen[len(projected)])
        for k in range(2):
            rows = slice(k * HALF, (k + 1) * HALF)
            hi, lo = x_hi[level], x_lo[level]
            part[level, rows] = (jnp.dot(b_hi[rows], hi, preferred_element_type=F32)
                                 + jnp.dot(b_hi[rows], lo, preferred_element_type=F32)
                                 + jnp.dot(b_lo[rows], hi, preferred_element_type=F32))

    def nt(a, b):
        return lax.dot_general(a, b, (((1,), (1,)), ((), ())), preferred_element_type=F32)

    state = {"applied": 0}

    tiles = [(0, V, 0), (0, V, 256), (0, V // 2, 512), (V // 2, V // 2, 512)]

    def apply(level, coefficients):
        first, last = state["applied"] == 0, state["applied"] == LEVELS - 1
        state["applied"] += 1
        for k, (row, rows, col) in enumerate(tiles):
            rows, cols = slice(row, row + rows), slice(col, col + 256)
            hi, lo = split(coefficients(cols))
            image = nt(x_hi[level, rows], hi) + nt(x_hi[level, rows], lo) + nt(x_lo[level, rows], hi)
            if last:
                out[rows, cols] = acc[rows, cols] + image
            else:
                acc[rows, cols] = image if first else acc[rows, cols] + image

    def add_into(level, offset, rows, slots):
        where = pl.ds(aligned(offset), rows)
        total = part[level, where, :]
        for slot in slots:
            total = total + recv[pl.ds(slot, rows), :]
        part[level, where, :] = total

    def cores_in(level):
        first, sem = ex.slots(HALF), ex.sem()
        ex.send(ex.at(part, level, HALF - mine, HALF), ex.at(recv, None, first, HALF), sem, ex.other, level)
        yield
        ex.wait(HALF, sem)
        add_into(level, mine, HALF, [first])

    def cores_out(level, sem, offset=0, rows=HALF):
        block = ex.at(coef, level, mine + offset, rows)
        ex.send(block, block, sem, ex.other, level)

    def both_cores(level):
        sem = ex.sem()
        cores_out(level, sem)
        yield
        ex.wait(HALF, sem)

    def pair_in(level, base, rows, bit, other):
        first, sem = ex.slots(rows), ex.sem()
        ex.send(ex.at(part, level, base + (1 - bit) * rows, rows), ex.at(recv, None, first, rows), sem, other, level)
        yield
        ex.wait(rows, sem)
        add_into(level, base + bit * rows, rows, [first])

    def pair_out(level, base, rows, bit, other):
        sem = ex.sem()
        block = ex.at(coef, level, base + bit * rows, rows)
        ex.send(block, block, sem, other, level)
        yield
        ex.wait(rows, sem)

    def roots_sum(level, base, rows, count):
        if count == 3:
            places = [2 * r for r in range(3)]
            is_root, my_root = jnp.logical_and(lax.rem(z, 2) == 0, z < 6), z // 2
        else:
            places = [r + r // 3 for r in range(6)]
            is_root, my_root = lax.rem(z, 4) != 3, z - z // 4
        not_root = jnp.logical_not(is_root)
        first, sem, back = ex.slots((NZ - 1) * rows), ex.sem(), ex.sem()
        for r, place in enumerate(places):
            slot = jnp.maximum(lax.rem(z - place + NZ, NZ) - 1, 0)
            ex.send(ex.at(part, level, base + r * rows, rows), ex.at(recv, None, first + slot * rows, rows),
                    sem, at_z(place), (level, "in"), when=z != place, drain=False)
        yield
        where = base + jnp.where(is_root, my_root * rows, 0)

        @pl.when(is_root)
        def _():
            ex.wait((NZ - 1) * rows, sem)
            total = part[level, pl.ds(aligned(where), rows), :]
            for d in range(NZ - 1):
                total = total + recv[pl.ds(first + d * rows, rows), :]
            coef[level, pl.ds(aligned(where), rows), :] = total

        block = ex.at(coef, level, where, rows)
        for d in range(1, NZ):
            ex.send(block, block, back, at_z(lax.rem(z + d, NZ)), (level, "out"), when=is_root)
        yield
        sent = ex.group((level, "in"))[0]

        @pl.when(is_root)
        def _():
            ex.wait((count - 1) * rows, back)
            ex.wait_sent((count - 1) * rows, sent)

        @pl.when(not_root)
        def _():
            ex.wait(count * rows, back)
            ex.wait_sent(count * rows, sent)

    def ring_blocks(level, base, rows, n, pos, narrow):
        def block(ref, lev, d, skip, size):
            k = lax.rem(pos + d + n, n)
            if narrow:
                return ex.at(ref, lev, base + (k // 2) * rows + skip, size, lax.rem(k, 2) * 128)
            return ex.at(ref, lev, base + k * rows + skip, size)

        return block

    def chain_in(level, base, rows, n, pos, device, total, narrow=False):
        cut = rows // 16 * 8
        up, down = device(lax.rem(pos + 1, n)), device(lax.rem(pos + n - 1, n))
        block = ring_blocks(level, base, rows, n, pos, narrow)
        cols = 0 if narrow else None
        last_down, last_up, last_sem = ex.slots(rows), ex.slots(rows), ex.sem()
        for far in range(n // 2, 0, -1):
            n_up, n_down, skip = (cut, rows - cut, cut) if far == n // 2 else (rows, rows, 0)
            first, first_down, sem = last_down, last_up, last_sem
            if far > 1:
                first, first_down, sem = ex.slots(n_up), ex.slots(n_down), ex.sem()
            elif n == 4:
                n_up, n_down, skip = cut, rows - cut, cut
            from_down, from_up = ex.at(recv, None, first, n_up, cols), ex.at(recv, None, first_down, n_down, cols)
            if n == 4 and far == 1:
                from_up = ex.at(recv, None, first_down + skip, n_down, cols)
            ex.send(block(part, level, far, 0, n_up), from_down, sem, up, level)
            ex.send(block(part, level, -far, skip, n_down), from_up, sem, down, level)
            if n == 4 and far == 2:
                ex.send(block(part, level, 1, cut, rows - cut), ex.at(recv, None, last_down + cut, rows - cut, cols),
                        last_sem, up, level)
                ex.send(block(part, level, -1, 0, cut), ex.at(recv, None, last_up, cut, cols), last_sem, down, level)
            yield
            if far > 1:
                ex.wait(n_up + n_down, sem, narrow)
                own = block(part, level, far - 1, 0, n_up)
                own[...] = own[...] + from_down[...]
                own = block(part, level, 1 - far, skip, n_down)
                own[...] = own[...] + from_up[...]
        ex.wait(2 * rows, last_sem, narrow)
        from_down, from_up = ex.at(recv, None, last_down, rows, cols), ex.at(recv, None, last_up, rows, cols)
        block(total, level, 0, 0, rows)[...] = block(part, level, 0, 0, rows)[...] + from_down[...] + from_up[...]

    def chain_out(level, base, rows, n, pos, device, narrow=False):
        cut = rows // 16 * 8
        up, down = device(lax.rem(pos + 1, n)), device(lax.rem(pos + n - 1, n))
        block = ring_blocks(level, base, rows, n, pos, narrow)

        def send(d, skip, size, sem, to):
            piece = block(coef, level, d, skip, size)
            ex.send(piece, piece, sem, to, level)

        if n == 4:
            sem, last_sem = ex.sem(), ex.sem()
            send(0, 0, cut, sem, up)
            send(0, cut, rows - cut, sem, down)
            send(0, cut, rows - cut, last_sem, up)
            send(0, 0, cut, last_sem, down)
            yield
            ex.wait(rows, sem, narrow)
            send(-1, 0, cut, last_sem, up)
            send(1, cut, rows - cut, last_sem, down)
            yield
            ex.wait(2 * rows, last_sem, narrow)
            return
        for far in range(1, n // 2 + 1):
            n_up, n_down, skip = (cut, rows - cut, cut) if far == n // 2 else (rows, rows, 0)
            sem = ex.sem()
            send(1 - far, 0, n_up, sem, up)
            send(far - 1, skip, n_down, sem, down)
            yield
            ex.wait(n_up + n_down, sem, narrow)

    def quad_sum(level, base, rows):
        place = lax.rem(z, 4)
        side = place // 2
        start = z - place
        middle = jnp.logical_or(place == 1, place == 2)
        edge = jnp.logical_not(middle)
        my_middle, my_edge, far_middle = at_z(start + 1 + side), at_z(start + 3 * side), at_z(start + 2 - side)
        near, far = base + side * rows, base + (1 - side) * rows
        first, sems = ex.slots(3 * rows), [ex.sem() for _ in range(3)]
        slot = [ex.at(recv, None, first + k * rows, rows) for k in range(3)]
        ex.send(ex.at(part, level, far, rows), slot[0], sems[0], my_middle, (level, "edge"), when=edge)
        ex.send(ex.at(part, level, near, rows), slot[1], sems[1], my_middle, (level, "edge"), when=edge)
        yield

        @pl.when(middle)
        def _():
            ex.wait(rows, sems[0])
            add_into(level, far, rows, [first])

        ex.send(ex.at(part, level, far, rows), slot[2], sems[1], far_middle, (level, "middle"), when=middle)
        yield

        @pl.when(middle)
        def _():
            ex.wait(2 * rows, sems[1])
            where = pl.ds(aligned(near), rows)
            coef[level, where, :] = (part[level, where, :] + recv[pl.ds(first + rows, rows), :]
                                     + recv[pl.ds(first + 2 * rows, rows), :])

        block, other = ex.at(coef, level, near, rows), ex.at(coef, level, far, rows)
        ex.send(block, block, sems[2], far_middle, (level, "middle"), when=middle)
        ex.send(block, block, sems[2], my_edge, (level, "middle"), when=middle)
        yield

        @pl.when(middle)
        def _():
            ex.wait(rows, sems[2])

        ex.send(other, other, sems[2], my_edge, (level, "middle"), when=middle)
        yield

        @pl.when(edge)
        def _():
            ex.wait(2 * rows, sems[2])

    def level_0():
        project(0)
        yield
        apply(0, lambda rows: part[0, rows])

    def level_1():
        project(1)
        first, sem = ex.slots(R), ex.sem()
        ex.send(part.at[1], ex.at(recv, None, first, R), sem, ex.other, 1)
        yield
        ex.wait(R, sem)
        apply(1, lambda rows: part[1, rows] + recv[first + rows.start:first + rows.stop, :])

    arrived = {2: ex.sem(), 3: ex.sem()}

    def level_2():
        project(2)
        yield from cores_in(2)
        yield
        ex.wait(HALF, arrived[2])
        apply(2, lambda rows: coef[2, rows])

    def chunk_2(k):
        rows = HALF // 4
        first, sem = ex.slots(rows), ex.sem()
        other = at_z(z + 1 - 2 * lax.rem(z, 2))
        ex.send(ex.at(part, 2, mine + k * rows, rows), ex.at(recv, None, first, rows), sem, other, 2)
        yield
        ex.wait(rows, sem)
        own = pl.ds(aligned(mine + k * rows), rows)
        coef[2, own, :] = part[2, own, :] + recv[pl.ds(first, rows), :]
        cores_out(2, arrived[2], k * rows, rows)

    def level_3():
        project(3)
        yield from cores_in(3)
        yield
        ex.wait(HALF, arrived[3])
        apply(3, lambda rows: coef[3, rows])

    def chunk_3(k):
        rows = HALF // 2
        yield from quad_sum(3, mine + k * rows, rows // 2)
        cores_out(3, arrived[3], k * rows, rows)

    def level_4():
        project(4)
        yield from cores_in(4)
        yield from chain_in(4, mine, HALF // NZ, NZ, z, at_z, coef)
        yield from chain_out(4, mine, HALF // NZ, NZ, z, at_z)
        yield from both_cores(4)
        apply(4, lambda rows: coef[4, rows])

    def level_5():
        project(5)
        yield from cores_in(5)
        bit = lax.rem(y, 2)
        other = at_y(y + 1 - 2 * bit)
        yield from pair_in(5, mine, HALF // 2, bit, other)
        base, rows = mine + bit * (HALF // 2), HALF // 2 // NZ
        yield from chain_in(5, base, rows, NZ, z, at_z, coef)
        yield from chain_out(5, base, rows, NZ, z, at_z)
        yield from pair_out(5, mine, HALF // 2, bit, other)
        yield from both_cores(5)
        apply(5, lambda rows: coef[5, rows])

    def level_6():
        project(6)
        yield from cores_in(6)
        yield from chain_in(6, mine, HALF // NY, NY, y, at_y, part)
        base, rows = mine + y * (HALF // NY), HALF // NY // NZ * 2
        yield from chain_in(6, base, rows, NZ, z, at_z, coef, narrow=True)
        yield from chain_out(6, base, rows, NZ, z, at_z, narrow=True)
        yield from chain_out(6, mine, HALF // NY, NY, y, at_y)
        yield from both_cores(6)
        apply(6, lambda rows: coef[6, rows])

    def level_7():
        project(7)
        yield from cores_in(7)
        bit = lax.rem(x, 2)
        other = at_x(x + 1 - 2 * bit)
        yield from pair_in(7, mine, HALF // 2, bit, other)
        base, rows = mine + bit * (HALF // 2), HALF // 2 // NY
        yield from chain_in(7, base, rows, NY, y, at_y, part)
        yield from roots_sum(7, base + y * rows, rows // 6, 6)
        yield from chain_out(7, base, rows, NY, y, at_y)
        yield from pair_out(7, mine, HALF // 2, bit, other)
        yield from both_cores(7)
        apply(7, lambda rows: coef[7, rows])

    def level_8():
        project(8)
        yield from cores_in(8)
        yield from chain_in(8, mine, HALF // NX, NX, x, at_x, part)
        base, rows = mine + x * (HALF // NX), HALF // NX // NY
        yield from chain_in(8, base, rows, NY, y, at_y, part)
        yield from roots_sum(8, base + y * rows, rows // 3, 3)
        yield from chain_out(8, base, rows, NY, y, at_y)
        yield from chain_out(8, mine, HALF // NX, NX, x, at_x)
        yield from both_cores(8)
        apply(8, lambda rows: coef[8, rows])

    levels = dict(enumerate(
        f() for f in (level_0, level_1, level_2, level_3, level_4, level_5, level_6, level_7, level_8)))
    levels.update({20 + k: chunk_2(k) for k in range(4)})
    levels.update({30 + k: chunk_3(k) for k in range(2)})
    early = first_seen[:EARLY]
    for level in early:
        project(level)
    pl.semaphore_wait(barrier, len(partners))
    for level in ORDER:
        next(levels[level], None)
    for rest in levels.values():
        for _ in rest:
            assert False
    assert state["applied"] == LEVELS
    ex.drain()


def body(basis, rhs, depth):
    hbm = pl.BlockSpec(memory_space=pltpu.HBM)
    return pl.pallas_call(
        kernel,
        out_shape=jax.ShapeDtypeStruct((V, R), F32),
        in_specs=[hbm, hbm, pl.BlockSpec(memory_space=pltpu.VMEM)],
        out_specs=pl.BlockSpec(memory_space=pltpu.VMEM),
        scratch_shapes=[
            pltpu.VMEM((LEVELS, V, S), F32),
            pltpu.VMEM((V, R), F32),
            pltpu.VMEM((LEVELS, V, S), BF16),
            pltpu.VMEM((LEVELS, V, S), BF16),
            pltpu.VMEM((R, V), BF16),
            pltpu.VMEM((R, V), BF16),
            pltpu.VMEM((V, 128), F32),
            pltpu.VMEM((LEVELS, R, S), F32),
            pltpu.VMEM((LEVELS, R, S), F32),
            pltpu.VMEM((RECV_ROWS, S), F32),
            pltpu.VMEM((V, R), F32),
            pltpu.SemaphoreType.DMA((LEVELS + 1,)),
            pltpu.SemaphoreType.DMA((N_SEND,)),
            pltpu.SemaphoreType.DMA((N_RECV,)),
        ],
        compiler_params=pltpu.CompilerParams(
            collective_id=0, has_side_effects=True, vmem_limit_bytes=52 * 1024 * 1024),
        name="coarse_solve",
    )(basis, rhs, depth.reshape(1, V))


def solution(mesh):
    in_specs = (P(None, "leaf", None), P("leaf", None), P("leaf"))
    out_specs = P("leaf", None)
    return jax.shard_map(body, mesh=mesh, in_specs=in_specs, out_specs=out_specs, check_vma=False)
```

```python
import functools

import jax
import jax.numpy as jnp
from jax import lax
from jax.experimental import pallas as pl
from jax.experimental.pallas import tpu as pltpu
from jax.sharding import PartitionSpec as P

MESH = pl.DeviceIdType.MESH
F32, BF16 = jnp.float32, jnp.bfloat16

S, V, R = 256, 512, 768
HALF = R // 2
NX, NY, NZ = 4, 4, 8
LEVELS = 9
EARLY = 2
RECV_ROWS, N_SEND, N_RECV = 6400, 20, 112

ORDER = [6, 7, 3, 5, 6, 8, 7, 3, 31, 0, 5, 4, 2, 6, 4, 8, 2, 22, 31, 7, 4, 8, 5, 6, 23, 22, 7, 5, 8, 6, 7, 8, 5, 6, 4,
         7, 8, 5, 6, 30, 31, 6, 7, 8, 1, 4, 31, 0, 5, 6, 7, 8, 4, 6, 23, 5, 7, 8, 4, 6, 5, 21, 7, 30, 8, 6, 7, 5, 4,
         20, 8, 1, 30, 6, 5, 8, 4, 30, 6, 7, 21, 20, 8, 4, 31, 6, 7, 5, 2, 30, 4, 8, 5, 3, 8]


def split(x):
    hi = x.astype(BF16)
    return hi, (x - hi.astype(F32)).astype(BF16)


def aligned(offset, by=8):
    return offset if isinstance(offset, int) else pl.multiple_of(offset, by)


class Exchange:
    def __init__(self, recv, send_sem, recv_sem, other):
        self.recv, self.send_sem, self.recv_sem, self.other = recv, send_sem, recv_sem, other
        self.rows = self.sends = self.recvs = 0
        self.sent = {}

    def slots(self, rows):
        first = self.rows
        self.rows += rows
        assert self.rows <= RECV_ROWS
        return first

    def sem(self):
        self.recvs += 1
        assert self.recvs <= N_RECV
        return self.recv_sem.at[self.recvs - 1]

    def at(self, ref, level, offset, rows, cols=None):
        where = (pl.ds(aligned(offset), rows),)
        if cols is not None:
            where += (pl.ds(aligned(cols, 128), 128),)
        return ref.at[where] if level is None else ref.at[(level,) + where]

    def group(self, key):
        if key not in self.sent:
            assert self.sends < N_SEND
            self.sent[key] = [self.send_sem.at[self.sends], 0, None]
            self.sends += 1
        return self.sent[key]

    def send(self, src, dst, sem, device, key, when=None, drain=True):
        group = self.group(key)
        copy = pltpu.make_async_remote_copy(
            src_ref=src, dst_ref=dst, send_sem=group[0], recv_sem=sem, device_id=(device,), device_id_type=MESH)
        if drain:
            group[1] += src.shape[0] * src.shape[1] // 128
            group[2] = when
        if when is None:
            copy.start()
        else:
            pl.when(when)(copy.start)

    def whole(self, halves):
        if halves % 16:
            return self.recv.at[pl.ds(0, halves), pl.ds(0, 128)]
        return self.recv.at[pl.ds(0, halves // 2)]

    def descriptor(self, halves, send_sem, recv_sem):
        ref = self.whole(halves)
        return pltpu.make_async_remote_copy(
            src_ref=ref, dst_ref=ref, send_sem=send_sem, recv_sem=recv_sem, device_id=(self.other,),
            device_id_type=MESH)

    def wait(self, rows, sem, narrow=False):
        self.descriptor(rows if narrow else 2 * rows, self.send_sem.at[0], sem).wait_recv()

    def wait_sent(self, rows, sem, narrow=False):
        self.descriptor(rows if narrow else 2 * rows, sem, self.recv_sem.at[0]).wait_send()

    def drain(self):
        for sem, halves, when in self.sent.values():
            if halves:
                wait = self.descriptor(halves, sem, self.recv_sem.at[0]).wait_send
                wait() if when is None else pl.when(when)(wait)


def kernel(basis, rhs, depth, out, bas_v, rhs_v, x_hi, x_lo, b_hi, b_lo, tier, part, coef, recv, acc,
           load_sem, send_sem, recv_sem):
    me = lax.axis_index("leaf")
    core = lax.rem(me, 2)
    z = lax.rem(me // 2, NZ)
    y = lax.rem(me // (2 * NZ), NY)
    x = me // (2 * NZ * NY)

    def at_core(c):
        return me - core + c

    def at_z(k):
        return me + 2 * (k - z)

    def at_y(k):
        return me + 2 * NZ * (k - y)

    def at_x(k):
        return me + 2 * NZ * NY * (k - x)

    barrier = pltpu.get_barrier_semaphore()
    partners = [at_core(1 - core)]
    partners += [at_z(lax.rem(z + d, NZ)) for d in (1, 2, NZ - 2, NZ - 1)]
    partners += [at_y(lax.rem(y + d, NY)) for d in (1, NY - 1)]
    partners += [at_x(lax.rem(x + d, NX)) for d in (1, NX - 1)]
    for partner in partners:
        pl.semaphore_signal(barrier, inc=1, device_id=(partner,), device_id_type=MESH)

    first_seen = [level for level in dict.fromkeys(ORDER) if level < LEVELS]
    load_rhs = pltpu.make_async_copy(rhs, rhs_v, load_sem.at[LEVELS])
    load_rhs.start()
    loads = {}
    for level in first_seen:
        loads[level] = pltpu.make_async_copy(basis.at[level], bas_v.at[level], load_sem.at[level])
        loads[level].start()

    for k in range(V // 128):
        row = depth[0:1, 128 * k:128 * (k + 1)].astype(F32)
        tier[128 * k:128 * (k + 1), :] = jnp.broadcast_to(row, (128, 128)).T

    load_rhs.wait()
    for k in range(R // 128):
        hi, lo = split(rhs_v[:, 128 * k:128 * (k + 1)].T)
        b_hi[128 * k:128 * (k + 1), :] = hi
        b_lo[128 * k:128 * (k + 1), :] = lo

    ex = Exchange(recv, send_sem, recv_sem, at_core(1 - core))
    mine = core * HALF

    projected, prepared = set(), set()

    def prepare(level):
        if level in prepared:
            return
        prepared.add(level)
        loads[level].wait()
        for k in range(S // 128):
            cols = slice(128 * k, 128 * (k + 1))
            kept = jnp.where(tier[...] >= float(level), bas_v[level, :, cols], 0.0)
            hi, lo = split(kept)
            x_hi[level, :, cols] = hi
            x_lo[level, :, cols] = lo

    def project(level):
        if level in projected:
            return
        projected.add(level)
        prepare(level)
        if len(projected) < LEVELS:
            prepare(first_seen[len(projected)])
        for k in range(2):
            rows = slice(k * HALF, (k + 1) * HALF)
            hi, lo = x_hi[level], x_lo[level]
            part[level, rows] = (jnp.dot(b_hi[rows], hi, preferred_element_type=F32)
                                 + jnp.dot(b_hi[rows], lo, preferred_element_type=F32)
                                 + jnp.dot(b_lo[rows], hi, preferred_element_type=F32))

    def nt(a, b):
        return lax.dot_general(a, b, (((1,), (1,)), ((), ())), preferred_element_type=F32)

    state = {"applied": 0}

    tiles = [(0, V, 0), (0, V, 256), (0, V // 2, 512), (V // 2, V // 2, 512)]

    def apply(level, coefficients):
        first, last = state["applied"] == 0, state["applied"] == LEVELS - 1
        state["applied"] += 1
        for k, (row, rows, col) in enumerate(tiles):
            rows, cols = slice(row, row + rows), slice(col, col + 256)
            hi, lo = split(coefficients(cols))
            image = nt(x_hi[level, rows], hi) + nt(x_hi[level, rows], lo) + nt(x_lo[level, rows], hi)
            if last:
                out[rows, cols] = acc[rows, cols] + image
            else:
                acc[rows, cols] = image if first else acc[rows, cols] + image

    def add_into(level, offset, rows, slots):
        where = pl.ds(aligned(offset), rows)
        total = part[level, where, :]
        for slot in slots:
            total = total + recv[pl.ds(slot, rows), :]
        part[level, where, :] = total

    def cores_in(level):
        first, sem = ex.slots(HALF), ex.sem()
        ex.send(ex.at(part, level, HALF - mine, HALF), ex.at(recv, None, first, HALF), sem, ex.other, level)
        yield
        ex.wait(HALF, sem)
        add_into(level, mine, HALF, [first])

    def cores_out(level, sem, offset=0, rows=HALF):
        block = ex.at(coef, level, mine + offset, rows)
        ex.send(block, block, sem, ex.other, level)

    def both_cores(level):
        sem = ex.sem()
        cores_out(level, sem)
        yield
        ex.wait(HALF, sem)

    def pair_in(level, base, rows, bit, other):
        first, sem = ex.slots(rows), ex.sem()
        ex.send(ex.at(part, level, base + (1 - bit) * rows, rows), ex.at(recv, None, first, rows), sem, other, level)
        yield
        ex.wait(rows, sem)
        add_into(level, base + bit * rows, rows, [first])

    def pair_out(level, base, rows, bit, other):
        sem = ex.sem()
        block = ex.at(coef, level, base + bit * rows, rows)
        ex.send(block, block, sem, other, level)
        yield
        ex.wait(rows, sem)

    def tree_sum(level, base, rows, narrow=False):
        def role(d):
            root = lax.rem(z - d + NZ, NZ)
            return lax.rem(root, 4) != 3, root - root // 4

        def block(ref, k):
            if narrow:
                return ex.at(ref, level, base + (k // 2) * rows, rows, lax.rem(k, 2) * 128)
            return ex.at(ref, level, base + k * rows, rows)

        def ahead(d):
            return at_z(lax.rem(z + d + NZ, NZ))

        def others(wait):
            for there, count in ((lax.rem(z, 4) == 3, 4), (lax.rem(z, 4) == 1, 5), (lax.rem(z, 2) == 0, 3)):
                pl.when(there)(functools.partial(wait, count * rows))

        first = ex.slots(7 * rows)
        slot = [ex.at(recv, None, first + k * rows, rows, 0 if narrow else None) for k in range(7)]
        sem_below, sem_above, sem_root, back_below, back_above, back = [ex.sem() for _ in range(6)]
        for d, to, k, sem in ((4, 2, 0, sem_below), (5, 1, 1, sem_below), (3, -1, 2, sem_above),
                              (7, 1, 3, sem_root), (1, -1, 4, sem_root)):
            there, mine_of = role(d)
            ex.send(block(part, mine_of), slot[k], sem, ahead(to), (level, "others"), when=there, drain=False)
        yield
        for d, count, slots, sem, to, k in ((6, 2, (0, 1), sem_below, 2, 5), (2, 1, (2,), sem_above, -2, 6)):
            there, mine_of = role(d)

            @pl.when(there)
            def _():
                ex.wait(count * rows, sem, narrow)
                total = block(part, mine_of)[...]
                for slot_at in slots:
                    total = total + slot[slot_at][...]
                block(part, mine_of)[...] = total

            ex.send(block(part, mine_of), slot[k], sem_root, ahead(to), (level, d), when=there)
        yield
        there, mine_of = role(0)

        @pl.when(there)
        def _():
            ex.wait(4 * rows, sem_root, narrow)
            total = block(part, mine_of)[...]
            for k in range(3, 7):
                total = total + slot[k][...]
            block(coef, mine_of)[...] = total

        piece = block(coef, mine_of)
        for to, sem in ((2, back_above), (-2, back_below), (1, back), (-1, back)):
            ex.send(piece, piece, sem, ahead(to), (level, 0), when=there)
        yield
        for d, sem, targets in ((6, back_below, (-2, -1)), (2, back_above, (1,))):
            there, mine_of = role(d)
            pl.when(there)(functools.partial(ex.wait, rows, sem, narrow))
            piece = block(coef, mine_of)
            for to in targets:
                ex.send(piece, piece, back, ahead(to), (level, d), when=there)
        yield
        others(lambda count: ex.wait(count, back, narrow))
        others(lambda count: ex.wait_sent(count, ex.group((level, "others"))[0], narrow))

    def ring_blocks(level, base, rows, n, pos, narrow):
        def block(ref, lev, d, skip, size):
            k = lax.rem(pos + d + n, n)
            if narrow:
                return ex.at(ref, lev, base + (k // 2) * rows + skip, size, lax.rem(k, 2) * 128)
            return ex.at(ref, lev, base + k * rows + skip, size)

        return block

    def chain_in(level, base, rows, n, pos, device, total, narrow=False):
        cut = rows // 16 * 8
        up, down = device(lax.rem(pos + 1, n)), device(lax.rem(pos + n - 1, n))
        block = ring_blocks(level, base, rows, n, pos, narrow)
        cols = 0 if narrow else None
        last_down, last_up, last_sem = ex.slots(rows), ex.slots(rows), ex.sem()
        for far in range(n // 2, 0, -1):
            n_up, n_down, skip = (cut, rows - cut, cut) if far == n // 2 else (rows, rows, 0)
            first, first_down, sem = last_down, last_up, last_sem
            if far > 1:
                first, first_down, sem = ex.slots(n_up), ex.slots(n_down), ex.sem()
            elif n == 4:
                n_up, n_down, skip = cut, rows - cut, cut
            from_down, from_up = ex.at(recv, None, first, n_up, cols), ex.at(recv, None, first_down, n_down, cols)
            if n == 4 and far == 1:
                from_up = ex.at(recv, None, first_down + skip, n_down, cols)
            ex.send(block(part, level, far, 0, n_up), from_down, sem, up, level)
            ex.send(block(part, level, -far, skip, n_down), from_up, sem, down, level)
            if n == 4 and far == 2:
                ex.send(block(part, level, 1, cut, rows - cut), ex.at(recv, None, last_down + cut, rows - cut, cols),
                        last_sem, up, level)
                ex.send(block(part, level, -1, 0, cut), ex.at(recv, None, last_up, cut, cols), last_sem, down, level)
            yield
            if far > 1:
                ex.wait(n_up + n_down, sem, narrow)
                own = block(part, level, far - 1, 0, n_up)
                own[...] = own[...] + from_down[...]
                own = block(part, level, 1 - far, skip, n_down)
                own[...] = own[...] + from_up[...]
        ex.wait(2 * rows, last_sem, narrow)
        from_down, from_up = ex.at(recv, None, last_down, rows, cols), ex.at(recv, None, last_up, rows, cols)
        block(total, level, 0, 0, rows)[...] = block(part, level, 0, 0, rows)[...] + from_down[...] + from_up[...]

    def chain_out(level, base, rows, n, pos, device, narrow=False):
        cut = rows // 16 * 8
        up, down = device(lax.rem(pos + 1, n)), device(lax.rem(pos + n - 1, n))
        block = ring_blocks(level, base, rows, n, pos, narrow)

        def send(d, skip, size, sem, to):
            piece = block(coef, level, d, skip, size)
            ex.send(piece, piece, sem, to, level)

        if n == 4:
            sem, last_sem = ex.sem(), ex.sem()
            send(0, 0, cut, sem, up)
            send(0, cut, rows - cut, sem, down)
            send(0, cut, rows - cut, last_sem, up)
            send(0, 0, cut, last_sem, down)
            yield
            ex.wait(rows, sem, narrow)
            send(-1, 0, cut, last_sem, up)
            send(1, cut, rows - cut, last_sem, down)
            yield
            ex.wait(2 * rows, last_sem, narrow)
            return
        for far in range(1, n // 2 + 1):
            n_up, n_down, skip = (cut, rows - cut, cut) if far == n // 2 else (rows, rows, 0)
            sem = ex.sem()
            send(1 - far, 0, n_up, sem, up)
            send(far - 1, skip, n_down, sem, down)
            yield
            ex.wait(n_up + n_down, sem, narrow)

    def quad_sum(level, base, rows):
        place = lax.rem(z, 4)
        side = place // 2
        start = z - place
        middle = jnp.logical_or(place == 1, place == 2)
        edge = jnp.logical_not(middle)
        my_middle, my_edge, far_middle = at_z(start + 1 + side), at_z(start + 3 * side), at_z(start + 2 - side)
        near, far = base + side * rows, base + (1 - side) * rows
        first, sems = ex.slots(3 * rows), [ex.sem() for _ in range(3)]
        slot = [ex.at(recv, None, first + k * rows, rows) for k in range(3)]
        ex.send(ex.at(part, level, far, rows), slot[0], sems[0], my_middle, (level, "edge"), when=edge)
        ex.send(ex.at(part, level, near, rows), slot[1], sems[1], my_middle, (level, "edge"), when=edge)
        yield

        @pl.when(middle)
        def _():
            ex.wait(rows, sems[0])
            add_into(level, far, rows, [first])

        ex.send(ex.at(part, level, far, rows), slot[2], sems[1], far_middle, (level, "middle"), when=middle)
        yield

        @pl.when(middle)
        def _():
            ex.wait(2 * rows, sems[1])
            where = pl.ds(aligned(near), rows)
            coef[level, where, :] = (part[level, where, :] + recv[pl.ds(first + rows, rows), :]
                                     + recv[pl.ds(first + 2 * rows, rows), :])

        block, other = ex.at(coef, level, near, rows), ex.at(coef, level, far, rows)
        ex.send(block, block, sems[2], far_middle, (level, "middle"), when=middle)
        ex.send(block, block, sems[2], my_edge, (level, "middle"), when=middle)
        yield

        @pl.when(middle)
        def _():
            ex.wait(rows, sems[2])

        ex.send(other, other, sems[2], my_edge, (level, "middle"), when=middle)
        yield

        @pl.when(edge)
        def _():
            ex.wait(2 * rows, sems[2])

    def level_0():
        project(0)
        yield
        apply(0, lambda rows: part[0, rows])

    def level_1():
        project(1)
        first, sem = ex.slots(R), ex.sem()
        ex.send(part.at[1], ex.at(recv, None, first, R), sem, ex.other, 1)
        yield
        ex.wait(R, sem)
        apply(1, lambda rows: part[1, rows] + recv[first + rows.start:first + rows.stop, :])

    arrived = {2: ex.sem(), 3: ex.sem()}

    def level_2():
        project(2)
        yield from cores_in(2)
        yield
        ex.wait(HALF, arrived[2])
        apply(2, lambda rows: coef[2, rows])

    def chunk_2(k):
        rows = HALF // 4
        first, sem = ex.slots(rows), ex.sem()
        other = at_z(z + 1 - 2 * lax.rem(z, 2))
        ex.send(ex.at(part, 2, mine + k * rows, rows), ex.at(recv, None, first, rows), sem, other, 2)
        yield
        ex.wait(rows, sem)
        own = pl.ds(aligned(mine + k * rows), rows)
        coef[2, own, :] = part[2, own, :] + recv[pl.ds(first, rows), :]
        cores_out(2, arrived[2], k * rows, rows)

    def level_3():
        project(3)
        yield from cores_in(3)
        yield
        ex.wait(HALF, arrived[3])
        apply(3, lambda rows: coef[3, rows])

    def chunk_3(k):
        rows = HALF // 2
        yield from quad_sum(3, mine + k * rows, rows // 2)
        cores_out(3, arrived[3], k * rows, rows)

    def level_4():
        project(4)
        yield from cores_in(4)
        yield from chain_in(4, mine, HALF // NZ, NZ, z, at_z, coef)
        yield from chain_out(4, mine, HALF // NZ, NZ, z, at_z)
        yield from both_cores(4)
        apply(4, lambda rows: coef[4, rows])

    def level_5():
        project(5)
        yield from cores_in(5)
        bit = lax.rem(y, 2)
        other = at_y(y + 1 - 2 * bit)
        yield from pair_in(5, mine, HALF // 2, bit, other)
        base, rows = mine + bit * (HALF // 2), HALF // 2 // NZ
        yield from chain_in(5, base, rows, NZ, z, at_z, coef)
        yield from chain_out(5, base, rows, NZ, z, at_z)
        yield from pair_out(5, mine, HALF // 2, bit, other)
        yield from both_cores(5)
        apply(5, lambda rows: coef[5, rows])

    def level_6():
        project(6)
        yield from cores_in(6)
        yield from chain_in(6, mine, HALF // NY, NY, y, at_y, part)
        base, rows = mine + y * (HALF // NY), HALF // NY // NZ * 2
        yield from chain_in(6, base, rows, NZ, z, at_z, coef, narrow=True)
        yield from chain_out(6, base, rows, NZ, z, at_z, narrow=True)
        yield from chain_out(6, mine, HALF // NY, NY, y, at_y)
        yield from both_cores(6)
        apply(6, lambda rows: coef[6, rows])

    def level_7():
        project(7)
        yield from cores_in(7)
        bit = lax.rem(x, 2)
        other = at_x(x + 1 - 2 * bit)
        yield from pair_in(7, mine, HALF // 2, bit, other)
        base, rows = mine + bit * (HALF // 2), HALF // 2 // NY
        yield from chain_in(7, base, rows, NY, y, at_y, part)
        yield from tree_sum(7, base + y * rows, rows // 6)
        yield from chain_out(7, base, rows, NY, y, at_y)
        yield from pair_out(7, mine, HALF // 2, bit, other)
        yield from both_cores(7)
        apply(7, lambda rows: coef[7, rows])

    def level_8():
        project(8)
        yield from cores_in(8)
        yield from chain_in(8, mine, HALF // NX, NX, x, at_x, part)
        base, rows = mine + x * (HALF // NX), HALF // NX // NY
        yield from chain_in(8, base, rows, NY, y, at_y, part)
        yield from tree_sum(8, base + y * rows, rows // 3, narrow=True)
        yield from chain_out(8, base, rows, NY, y, at_y)
        yield from chain_out(8, mine, HALF // NX, NX, x, at_x)
        yield from both_cores(8)
        apply(8, lambda rows: coef[8, rows])

    levels = dict(enumerate(
        f() for f in (level_0, level_1, level_2, level_3, level_4, level_5, level_6, level_7, level_8)))
    levels.update({20 + k: chunk_2(k) for k in range(4)})
    levels.update({30 + k: chunk_3(k) for k in range(2)})
    early = first_seen[:EARLY]
    for level in early:
        project(level)
    pl.semaphore_wait(barrier, len(partners))
    for level in ORDER:
        next(levels[level], None)
    for rest in levels.values():
        for _ in rest:
            assert False
    assert state["applied"] == LEVELS
    ex.drain()


def body(basis, rhs, depth):
    hbm = pl.BlockSpec(memory_space=pltpu.HBM)
    return pl.pallas_call(
        kernel,
        out_shape=jax.ShapeDtypeStruct((V, R), F32),
        in_specs=[hbm, hbm, pl.BlockSpec(memory_space=pltpu.VMEM)],
        out_specs=pl.BlockSpec(memory_space=pltpu.VMEM),
        scratch_shapes=[
            pltpu.VMEM((LEVELS, V, S), F32),
            pltpu.VMEM((V, R), F32),
            pltpu.VMEM((LEVELS, V, S), BF16),
            pltpu.VMEM((LEVELS, V, S), BF16),
            pltpu.VMEM((R, V), BF16),
            pltpu.VMEM((R, V), BF16),
            pltpu.VMEM((V, 128), F32),
            pltpu.VMEM((LEVELS, R, S), F32),
            pltpu.VMEM((LEVELS, R, S), F32),
            pltpu.VMEM((RECV_ROWS, S), F32),
            pltpu.VMEM((V, R), F32),
            pltpu.SemaphoreType.DMA((LEVELS + 1,)),
            pltpu.SemaphoreType.DMA((N_SEND,)),
            pltpu.SemaphoreType.DMA((N_RECV,)),
        ],
        compiler_params=pltpu.CompilerParams(
            collective_id=0, has_side_effects=True, vmem_limit_bytes=52 * 1024 * 1024),
        name="coarse_solve",
    )(basis, rhs, depth.reshape(1, V))


def solution(mesh):
    in_specs = (P(None, "leaf", None), P("leaf", None), P("leaf"))
    out_specs = P("leaf", None)
    return jax.shard_map(body, mesh=mesh, in_specs=in_specs, out_specs=out_specs, check_vma=False)
```

```python
import functools

import jax
import jax.numpy as jnp
from jax import lax
from jax.experimental import pallas as pl
from jax.experimental.pallas import tpu as pltpu
from jax.sharding import PartitionSpec as P

MESH = pl.DeviceIdType.MESH
F32, BF16 = jnp.float32, jnp.bfloat16

S, V, R = 256, 512, 768
HALF = R // 2
NX, NY, NZ = 4, 4, 8
LEVELS = 9
EARLY = 2
RECV_ROWS, N_SEND, N_RECV = 6400, 24, 112

ORDER = [5, 3, 8, 6, 5, 3, 30, 8, 7, 2, 7, 6, 2, 21, 30, 4, 5, 1, 4, 22, 8, 6, 5, 7, 6, 31, 8, 7, 4, 1, 30, 6, 8, 0, 5,
         0, 8, 7, 4, 5, 8, 7, 6, 4, 5, 8, 7, 6, 4, 5, 8, 6, 7, 4, 5, 8, 20, 31, 7, 4, 8, 5, 6, 30, 7, 8, 4, 21, 5, 23,
         31, 7, 22, 4, 20, 6, 31, 8, 4, 23, 6, 5, 7, 30, 5, 31, 8, 2, 7, 3, 8]


def split(x):
    hi = x.astype(BF16)
    return hi, (x - hi.astype(F32)).astype(BF16)


def aligned(offset, by=8):
    return offset if isinstance(offset, int) else pl.multiple_of(offset, by)


class Exchange:
    def __init__(self, recv, send_sem, recv_sem, other):
        self.recv, self.send_sem, self.recv_sem, self.other = recv, send_sem, recv_sem, other
        self.rows = self.sends = self.recvs = 0
        self.sent = {}

    def slots(self, rows):
        first = self.rows
        self.rows += rows
        assert self.rows <= RECV_ROWS
        return first

    def sem(self):
        self.recvs += 1
        assert self.recvs <= N_RECV
        return self.recv_sem.at[self.recvs - 1]

    def at(self, ref, level, offset, rows, cols=None):
        where = (pl.ds(aligned(offset), rows),)
        if cols is not None:
            where += (pl.ds(aligned(cols, 128), 128),)
        return ref.at[where] if level is None else ref.at[(level,) + where]

    def group(self, key):
        if key not in self.sent:
            assert self.sends < N_SEND
            self.sent[key] = [self.send_sem.at[self.sends], 0, None]
            self.sends += 1
        return self.sent[key]

    def send(self, src, dst, sem, device, key, when=None, drain=True):
        group = self.group(key)
        copy = pltpu.make_async_remote_copy(
            src_ref=src, dst_ref=dst, send_sem=group[0], recv_sem=sem, device_id=(device,), device_id_type=MESH)
        if drain:
            group[1] += src.shape[0] * src.shape[1] // 128
            group[2] = when
        if when is None:
            copy.start()
        else:
            pl.when(when)(copy.start)

    def whole(self, halves):
        if halves % 16:
            return self.recv.at[pl.ds(0, halves), pl.ds(0, 128)]
        return self.recv.at[pl.ds(0, halves // 2)]

    def descriptor(self, halves, send_sem, recv_sem):
        ref = self.whole(halves)
        return pltpu.make_async_remote_copy(
            src_ref=ref, dst_ref=ref, send_sem=send_sem, recv_sem=recv_sem, device_id=(self.other,),
            device_id_type=MESH)

    def wait(self, rows, sem, narrow=False):
        self.descriptor(rows if narrow else 2 * rows, self.send_sem.at[0], sem).wait_recv()

    def wait_sent(self, rows, sem, narrow=False):
        self.descriptor(rows if narrow else 2 * rows, sem, self.recv_sem.at[0]).wait_send()

    def drain(self):
        for sem, halves, when in self.sent.values():
            if halves:
                wait = self.descriptor(halves, sem, self.recv_sem.at[0]).wait_send
                wait() if when is None else pl.when(when)(wait)


def kernel(basis, rhs, depth, out, bas_v, rhs_v, x_hi, x_lo, b_hi, b_lo, tier, part, coef, recv, acc,
           load_sem, send_sem, recv_sem):
    me = lax.axis_index("leaf")
    core = lax.rem(me, 2)
    z = lax.rem(me // 2, NZ)
    y = lax.rem(me // (2 * NZ), NY)
    x = me // (2 * NZ * NY)

    def at_core(c):
        return me - core + c

    def at_z(k):
        return me + 2 * (k - z)

    def at_y(k):
        return me + 2 * NZ * (k - y)

    def at_x(k):
        return me + 2 * NZ * NY * (k - x)

    barrier = pltpu.get_barrier_semaphore()
    partners = [at_core(1 - core)]
    partners += [at_z(lax.rem(z + d, NZ)) for d in (1, 2, NZ - 2, NZ - 1)]
    partners += [at_y(lax.rem(y + d, NY)) for d in (1, NY - 1)]
    partners += [at_x(lax.rem(x + d, NX)) for d in (1, NX - 1)]
    for partner in partners:
        pl.semaphore_signal(barrier, inc=1, device_id=(partner,), device_id_type=MESH)

    first_seen = [level for level in dict.fromkeys(ORDER) if level < LEVELS]
    load_rhs = pltpu.make_async_copy(rhs, rhs_v, load_sem.at[LEVELS])
    load_rhs.start()
    loads = {}
    for level in first_seen:
        loads[level] = pltpu.make_async_copy(basis.at[level], bas_v.at[level], load_sem.at[level])
        loads[level].start()

    for k in range(V // 128):
        row = depth[0:1, 128 * k:128 * (k + 1)].astype(F32)
        tier[128 * k:128 * (k + 1), :] = jnp.broadcast_to(row, (128, 128)).T

    load_rhs.wait()
    for k in range(R // 128):
        hi, lo = split(rhs_v[:, 128 * k:128 * (k + 1)].T)
        b_hi[128 * k:128 * (k + 1), :] = hi
        b_lo[128 * k:128 * (k + 1), :] = lo

    ex = Exchange(recv, send_sem, recv_sem, at_core(1 - core))
    mine = core * HALF

    projected, prepared = set(), set()

    def prepare(level):
        if level in prepared:
            return
        prepared.add(level)
        loads[level].wait()
        for k in range(S // 128):
            cols = slice(128 * k, 128 * (k + 1))
            kept = jnp.where(tier[...] >= float(level), bas_v[level, :, cols], 0.0)
            hi, lo = split(kept)
            x_hi[level, :, cols] = hi
            x_lo[level, :, cols] = lo

    def project(level):
        if level in projected:
            return
        projected.add(level)
        prepare(level)
        if len(projected) < LEVELS:
            prepare(first_seen[len(projected)])
        for k in range(2):
            rows = slice(k * HALF, (k + 1) * HALF)
            hi, lo = x_hi[level], x_lo[level]
            part[level, rows] = (jnp.dot(b_hi[rows], hi, preferred_element_type=F32)
                                 + jnp.dot(b_hi[rows], lo, preferred_element_type=F32)
                                 + jnp.dot(b_lo[rows], hi, preferred_element_type=F32))

    def nt(a, b):
        return lax.dot_general(a, b, (((1,), (1,)), ((), ())), preferred_element_type=F32)

    state = {"applied": 0}

    tiles = [(0, V, 0), (0, V, 256), (0, V // 2, 512), (V // 2, V // 2, 512)]

    def apply(level, coefficients):
        first, last = state["applied"] == 0, state["applied"] == LEVELS - 1
        state["applied"] += 1
        for k, (row, rows, col) in enumerate(tiles):
            rows, cols = slice(row, row + rows), slice(col, col + 256)
            hi, lo = split(coefficients(cols))
            image = nt(x_hi[level, rows], hi) + nt(x_hi[level, rows], lo) + nt(x_lo[level, rows], hi)
            if last:
                out[rows, cols] = acc[rows, cols] + image
            else:
                acc[rows, cols] = image if first else acc[rows, cols] + image

    def add_into(level, offset, rows, slots):
        where = pl.ds(aligned(offset), rows)
        total = part[level, where, :]
        for slot in slots:
            total = total + recv[pl.ds(slot, rows), :]
        part[level, where, :] = total

    def cores_in(level):
        first, sem = ex.slots(HALF), ex.sem()
        ex.send(ex.at(part, level, HALF - mine, HALF), ex.at(recv, None, first, HALF), sem, ex.other, level)
        yield
        ex.wait(HALF, sem)
        add_into(level, mine, HALF, [first])

    def cores_out(level, sem, offset=0, rows=HALF):
        block = ex.at(coef, level, mine + offset, rows)
        ex.send(block, block, sem, ex.other, level)

    def both_cores(level):
        sem = ex.sem()
        cores_out(level, sem)
        yield
        ex.wait(HALF, sem)

    def pair_in(level, base, rows, bit, other):
        first, sem = ex.slots(rows), ex.sem()
        ex.send(ex.at(part, level, base + (1 - bit) * rows, rows), ex.at(recv, None, first, rows), sem, other, level)
        yield
        ex.wait(rows, sem)
        add_into(level, base + bit * rows, rows, [first])

    def pair_out(level, base, rows, bit, other):
        sem = ex.sem()
        block = ex.at(coef, level, base + bit * rows, rows)
        ex.send(block, block, sem, other, level)
        yield
        ex.wait(rows, sem)

    def tree_sum(level, base, rows, narrow=False):
        def role(d):
            root = lax.rem(z - d + NZ, NZ)
            return lax.rem(root, 4) != 3, root - root // 4

        def block(ref, k):
            if narrow:
                return ex.at(ref, level, base + (k // 2) * rows, rows, lax.rem(k, 2) * 128)
            return ex.at(ref, level, base + k * rows, rows)

        def ahead(d):
            return at_z(lax.rem(z + d + NZ, NZ))

        def others(wait):
            for there, count in ((lax.rem(z, 4) == 3, 4), (lax.rem(z, 4) == 1, 5), (lax.rem(z, 2) == 0, 3)):
                pl.when(there)(functools.partial(wait, count * rows))

        first = ex.slots(7 * rows)
        slot = [ex.at(recv, None, first + k * rows, rows, 0 if narrow else None) for k in range(7)]
        sem_below, sem_above, sem_root, back_below, back_above, back = [ex.sem() for _ in range(6)]
        for d, to, k, sem in ((4, 2, 0, sem_below), (5, 1, 1, sem_below), (3, -1, 2, sem_above),
                              (7, 1, 3, sem_root), (1, -1, 4, sem_root)):
            there, mine_of = role(d)
            ex.send(block(part, mine_of), slot[k], sem, ahead(to), (level, "others"), when=there, drain=False)
        yield
        for d, count, slots, sem, to, k in ((6, 2, (0, 1), sem_below, 2, 5), (2, 1, (2,), sem_above, -2, 6)):
            there, mine_of = role(d)

            @pl.when(there)
            def _():
                ex.wait(count * rows, sem, narrow)
                total = block(part, mine_of)[...]
                for slot_at in slots:
                    total = total + slot[slot_at][...]
                block(part, mine_of)[...] = total

            ex.send(block(part, mine_of), slot[k], sem_root, ahead(to), (level, d), when=there)
        yield
        there, mine_of = role(0)

        @pl.when(there)
        def _():
            ex.wait(4 * rows, sem_root, narrow)
            total = block(part, mine_of)[...]
            for k in range(3, 7):
                total = total + slot[k][...]
            block(coef, mine_of)[...] = total

        piece = block(coef, mine_of)
        for to, sem in ((2, back_above), (-2, back_below), (1, back), (-1, back)):
            ex.send(piece, piece, sem, ahead(to), (level, 0), when=there)
        yield
        for d, sem, targets in ((6, back_below, (-2, -1)), (2, back_above, (1,))):
            there, mine_of = role(d)
            pl.when(there)(functools.partial(ex.wait, rows, sem, narrow))
            piece = block(coef, mine_of)
            for to in targets:
                ex.send(piece, piece, back, ahead(to), (level, d), when=there)
        yield
        others(lambda count: ex.wait(count, back, narrow))
        others(lambda count: ex.wait_sent(count, ex.group((level, "others"))[0], narrow))

    def ring_blocks(level, base, rows, n, pos, narrow):
        def block(ref, lev, d, skip, size):
            k = lax.rem(pos + d + n, n)
            if narrow:
                return ex.at(ref, lev, base + (k // 2) * rows + skip, size, lax.rem(k, 2) * 128)
            return ex.at(ref, lev, base + k * rows + skip, size)

        return block

    def chain_in(level, base, rows, n, pos, device, total, narrow=False):
        cut = rows // 16 * 8
        up, down = device(lax.rem(pos + 1, n)), device(lax.rem(pos + n - 1, n))
        block = ring_blocks(level, base, rows, n, pos, narrow)
        cols = 0 if narrow else None
        last_down, last_up, last_sem = ex.slots(rows), ex.slots(rows), ex.sem()
        for far in range(n // 2, 0, -1):
            n_up, n_down, skip = (cut, rows - cut, cut) if far == n // 2 else (rows, rows, 0)
            first, first_down, sem = last_down, last_up, last_sem
            if far > 1:
                first, first_down, sem = ex.slots(n_up), ex.slots(n_down), ex.sem()
            elif n == 4:
                n_up, n_down, skip = cut, rows - cut, cut
            from_down, from_up = ex.at(recv, None, first, n_up, cols), ex.at(recv, None, first_down, n_down, cols)
            if n == 4 and far == 1:
                from_up = ex.at(recv, None, first_down + skip, n_down, cols)
            ex.send(block(part, level, far, 0, n_up), from_down, sem, up, level)
            ex.send(block(part, level, -far, skip, n_down), from_up, sem, down, level)
            if n == 4 and far == 2:
                ex.send(block(part, level, 1, cut, rows - cut), ex.at(recv, None, last_down + cut, rows - cut, cols),
                        last_sem, up, level)
                ex.send(block(part, level, -1, 0, cut), ex.at(recv, None, last_up, cut, cols), last_sem, down, level)
            yield
            if far > 1:
                ex.wait(n_up + n_down, sem, narrow)
                own = block(part, level, far - 1, 0, n_up)
                own[...] = own[...] + from_down[...]
                own = block(part, level, 1 - far, skip, n_down)
                own[...] = own[...] + from_up[...]
        ex.wait(2 * rows, last_sem, narrow)
        from_down, from_up = ex.at(recv, None, last_down, rows, cols), ex.at(recv, None, last_up, rows, cols)
        block(total, level, 0, 0, rows)[...] = block(part, level, 0, 0, rows)[...] + from_down[...] + from_up[...]

    def chain_out(level, base, rows, n, pos, device, narrow=False):
        cut = rows // 16 * 8
        up, down = device(lax.rem(pos + 1, n)), device(lax.rem(pos + n - 1, n))
        block = ring_blocks(level, base, rows, n, pos, narrow)

        def send(d, skip, size, sem, to):
            piece = block(coef, level, d, skip, size)
            ex.send(piece, piece, sem, to, level)

        if n == 4:
            sem, last_sem = ex.sem(), ex.sem()
            send(0, 0, cut, sem, up)
            send(0, cut, rows - cut, sem, down)
            send(0, cut, rows - cut, last_sem, up)
            send(0, 0, cut, last_sem, down)
            yield
            ex.wait(rows, sem, narrow)
            send(-1, 0, cut, last_sem, up)
            send(1, cut, rows - cut, last_sem, down)
            yield
            ex.wait(2 * rows, last_sem, narrow)
            return
        for far in range(1, n // 2 + 1):
            n_up, n_down, skip = (cut, rows - cut, cut) if far == n // 2 else (rows, rows, 0)
            sem = ex.sem()
            send(1 - far, 0, n_up, sem, up)
            send(far - 1, skip, n_down, sem, down)
            yield
            ex.wait(n_up + n_down, sem, narrow)

    def quad_sum(level, base, rows):
        place = lax.rem(z, 4)
        side = place // 2
        start = z - place
        middle = jnp.logical_or(place == 1, place == 2)
        edge = jnp.logical_not(middle)
        my_middle, my_edge, far_middle = at_z(start + 1 + side), at_z(start + 3 * side), at_z(start + 2 - side)
        near, far = base + side * rows, base + (1 - side) * rows
        first, sems = ex.slots(3 * rows), [ex.sem() for _ in range(3)]
        slot = [ex.at(recv, None, first + k * rows, rows) for k in range(3)]
        ex.send(ex.at(part, level, far, rows), slot[0], sems[0], my_middle, (level, "edge"), when=edge)
        ex.send(ex.at(part, level, near, rows), slot[1], sems[1], my_middle, (level, "edge"), when=edge)
        yield

        @pl.when(middle)
        def _():
            ex.wait(rows, sems[0])
            add_into(level, far, rows, [first])

        ex.send(ex.at(part, level, far, rows), slot[2], sems[1], far_middle, (level, "middle"), when=middle)
        yield

        @pl.when(middle)
        def _():
            ex.wait(2 * rows, sems[1])
            where = pl.ds(aligned(near), rows)
            coef[level, where, :] = (part[level, where, :] + recv[pl.ds(first + rows, rows), :]
                                     + recv[pl.ds(first + 2 * rows, rows), :])

        block, other = ex.at(coef, level, near, rows), ex.at(coef, level, far, rows)
        ex.send(block, block, sems[2], far_middle, (level, "middle"), when=middle)
        ex.send(block, block, sems[2], my_edge, (level, "middle"), when=middle)
        yield

        @pl.when(middle)
        def _():
            ex.wait(rows, sems[2])

        ex.send(other, other, sems[2], my_edge, (level, "middle"), when=middle)
        yield

        @pl.when(edge)
        def _():
            ex.wait(2 * rows, sems[2])

    def level_0():
        project(0)
        yield
        apply(0, lambda rows: part[0, rows])

    def level_1():
        project(1)
        first, sem = ex.slots(R), ex.sem()
        ex.send(part.at[1], ex.at(recv, None, first, R), sem, ex.other, 1)
        yield
        ex.wait(R, sem)
        apply(1, lambda rows: part[1, rows] + recv[first + rows.start:first + rows.stop, :])

    arrived = {2: ex.sem(), 3: ex.sem()}

    def level_2():
        project(2)
        yield from cores_in(2)
        yield
        ex.wait(HALF, arrived[2])
        apply(2, lambda rows: coef[2, rows])

    def chunk_2(k):
        rows = HALF // 4
        first, sem = ex.slots(rows), ex.sem()
        other = at_z(z + 1 - 2 * lax.rem(z, 2))
        ex.send(ex.at(part, 2, mine + k * rows, rows), ex.at(recv, None, first, rows), sem, other, 2)
        yield
        ex.wait(rows, sem)
        own = pl.ds(aligned(mine + k * rows), rows)
        coef[2, own, :] = part[2, own, :] + recv[pl.ds(first, rows), :]
        cores_out(2, arrived[2], k * rows, rows)

    def level_3():
        project(3)
        yield from cores_in(3)
        yield
        ex.wait(HALF, arrived[3])
        apply(3, lambda rows: coef[3, rows])

    def chunk_3(k):
        rows = HALF // 2
        yield from quad_sum(3, mine + k * rows, rows // 2)
        cores_out(3, arrived[3], k * rows, rows)

    def level_4():
        project(4)
        yield from cores_in(4)
        yield from chain_in(4, mine, HALF // NZ, NZ, z, at_z, coef)
        yield from chain_out(4, mine, HALF // NZ, NZ, z, at_z)
        yield from both_cores(4)
        apply(4, lambda rows: coef[4, rows])

    def level_5():
        project(5)
        yield from cores_in(5)
        bit = lax.rem(y, 2)
        other = at_y(y + 1 - 2 * bit)
        yield from pair_in(5, mine, HALF // 2, bit, other)
        base, rows = mine + bit * (HALF // 2), HALF // 2 // NZ
        yield from chain_in(5, base, rows, NZ, z, at_z, coef)
        yield from chain_out(5, base, rows, NZ, z, at_z)
        yield from pair_out(5, mine, HALF // 2, bit, other)
        yield from both_cores(5)
        apply(5, lambda rows: coef[5, rows])

    def level_6():
        project(6)
        yield from cores_in(6)
        yield from chain_in(6, mine, HALF // NY, NY, y, at_y, part)
        yield from tree_sum(6, mine + y * (HALF // NY), HALF // NY // 6)
        yield from chain_out(6, mine, HALF // NY, NY, y, at_y)
        yield from both_cores(6)
        apply(6, lambda rows: coef[6, rows])

    def level_7():
        project(7)
        yield from cores_in(7)
        bit = lax.rem(x, 2)
        other = at_x(x + 1 - 2 * bit)
        yield from pair_in(7, mine, HALF // 2, bit, other)
        base, rows = mine + bit * (HALF // 2), HALF // 2 // NY
        yield from chain_in(7, base, rows, NY, y, at_y, part)
        yield from tree_sum(7, base + y * rows, rows // 6)
        yield from chain_out(7, base, rows, NY, y, at_y)
        yield from pair_out(7, mine, HALF // 2, bit, other)
        yield from both_cores(7)
        apply(7, lambda rows: coef[7, rows])

    def level_8():
        project(8)
        yield from cores_in(8)
        yield from chain_in(8, mine, HALF // NX, NX, x, at_x, part)
        base, rows = mine + x * (HALF // NX), HALF // NX // NY
        yield from chain_in(8, base, rows, NY, y, at_y, part)
        yield from tree_sum(8, base + y * rows, rows // 3, narrow=True)
        yield from chain_out(8, base, rows, NY, y, at_y)
        yield from chain_out(8, mine, HALF // NX, NX, x, at_x)
        yield from both_cores(8)
        apply(8, lambda rows: coef[8, rows])

    levels = dict(enumerate(
        f() for f in (level_0, level_1, level_2, level_3, level_4, level_5, level_6, level_7, level_8)))
    levels.update({20 + k: chunk_2(k) for k in range(4)})
    levels.update({30 + k: chunk_3(k) for k in range(2)})
    early = first_seen[:EARLY]
    for level in early:
        project(level)
    pl.semaphore_wait(barrier, len(partners))
    for level in ORDER:
        next(levels[level], None)
    for rest in levels.values():
        for _ in rest:
            assert False
    assert state["applied"] == LEVELS
    ex.drain()


def body(basis, rhs, depth):
    hbm = pl.BlockSpec(memory_space=pltpu.HBM)
    return pl.pallas_call(
        kernel,
        out_shape=jax.ShapeDtypeStruct((V, R), F32),
        in_specs=[hbm, hbm, pl.BlockSpec(memory_space=pltpu.VMEM)],
        out_specs=pl.BlockSpec(memory_space=pltpu.VMEM),
        scratch_shapes=[
            pltpu.VMEM((LEVELS, V, S), F32),
            pltpu.VMEM((V, R), F32),
            pltpu.VMEM((LEVELS, V, S), BF16),
            pltpu.VMEM((LEVELS, V, S), BF16),
            pltpu.VMEM((R, V), BF16),
            pltpu.VMEM((R, V), BF16),
            pltpu.VMEM((V, 128), F32),
            pltpu.VMEM((LEVELS, R, S), F32),
            pltpu.VMEM((LEVELS, R, S), F32),
            pltpu.VMEM((RECV_ROWS, S), F32),
            pltpu.VMEM((V, R), F32),
            pltpu.SemaphoreType.DMA((LEVELS + 1,)),
            pltpu.SemaphoreType.DMA((N_SEND,)),
            pltpu.SemaphoreType.DMA((N_RECV,)),
        ],
        compiler_params=pltpu.CompilerParams(
            collective_id=0, has_side_effects=True, vmem_limit_bytes=52 * 1024 * 1024),
        name="coarse_solve",
    )(basis, rhs, depth.reshape(1, V))


def solution(mesh):
    in_specs = (P(None, "leaf", None), P("leaf", None), P("leaf"))
    out_specs = P("leaf", None)
    return jax.shard_map(body, mesh=mesh, in_specs=in_specs, out_specs=out_specs, check_vma=False)
```
